256 devices in a mesh: row: 8 (over x, y_lo), blk: 32 (over y_hi, z, core).
Axes of the slice: x: 4, y: 4 (y_hi: 2, y_lo: 2; y = y_hi * 2 + y_lo), z: 8, core: 2. Of those that a mesh axis runs over, the one named last changes fastest.
Arguments:
- elastic_kernel: bfloat16 [32, 1024, 8, 4096], P('blk', None, 'row'), may hold values from -0.046875 to 0.046875
- slip_deficit: float32 [32, 8, 128, 512], P('blk', 'row'), may hold values from -6 to 6
- state_variable: float32 [32, 8, 128, 512], P('blk', 'row'), may hold values from 0.2 to 5
- step_size: float32 [512], replicated, may hold values from 0.02 to 0.1
- load_stress: float32 [32, 8, 128], P('blk', 'row'), may hold values from -6 to 6
- normal_stress: float32 [32, 8, 128], P('blk', 'row'), may hold values from 0.5 to 2
- rate_table: float32 [16], replicated, may hold values from 0.3 to 1
- evolve_table: float32 [16], replicated, may hold values from 0.3 to 1.5
- patch_region: int32 [32, 8, 128], P('blk', 'row'), may hold values from 0 to 15
- creep_flag: int32 [32, 8, 128], P('blk', 'row'), may hold values 0 or 1
Outputs:
- velocity: float32 [32, 8, 128, 512], P('blk', 'row')
- deficit_out: float32 [32, 8, 128, 512], P('blk', 'row')
- state_out: float32 [32, 8, 128, 512], P('blk', 'row')
- step_next: float32 [512], replicated
The draws below stay inside these ranges and needn't reach their ends.
All inputs are finite; a program needn't handle non-finite values. Where the reference program divides by a largest or mean magnitude, that divisor is 1e-20 or more. No bound on the sum of `creep_flag` on one device may be relied on, other than what follows from the above.
Results may differ from the reference program's by a relative error of at most 0.0035.
Values may be sent and summed in bfloat16 or wider, within the bound.
No kernel may reach another device: no remote copies, remote signals or barrier semaphores. Data moves between devices by JAX's collectives and lax.ppermute only.
A program may use at most 64 MiB of HBM per device.

```python
import math
import jax
import jax.numpy as jnp
from jax import lax

ELEM_DEV = 128
MEMBERS = 512
REGIONS = 16
NEWTON = 3
STEPS = 2
ROW_GROUPS = 8
COL_BLOCKS = 32
ELEMENTS = 32768


def touch_ends(array, own_key, least, high):
    longest = array.shape.index(max(array.shape))
    spots = []
    for shift in (0, 1):
        where = [jax.random.randint(jax.random.fold_in(own_key, axis), (), 0, length) for axis, length in enumerate(array.shape)]
        where[longest] = (where[longest] + shift) % array.shape[longest]
        spots.append(tuple(where))
    return array.at[spots[0]].set(least).at[spots[1]].set(high)


def strengthened(array, key, source, target, blocks, factor):
    def block_of(dim):
        return (jnp.arange(array.shape[dim]) // (array.shape[dim] // blocks)).reshape((-1,) + (1,) * (array.ndim - 1 - dim))

    near = jax.random.permutation(key, blocks)[block_of(target)]
    far = (block_of(target) + blocks // 2) % blocks
    return jnp.where((block_of(source) == near) | (block_of(source) == far), factor * array, array)


def steps_of(own_key, extent, shards, least, top_value):
    def one(position, blocks):
        steps = jax.random.uniform(jax.random.fold_in(jax.random.fold_in(own_key, 6), position), (blocks,), jnp.float32, least / len(shards), top_value / len(shards))
        return jnp.repeat(jnp.exp(steps), extent[position] // blocks).reshape((-1,) + (1,) * (len(extent) - position - 1))

    gain = one(*shards[0])
    for cut in shards[1:]:
        gain = gain * one(*cut)
    return gain


def gaussian(rng, shape, width, reach, pieces=(), kind=jnp.bfloat16):
    values = jax.random.normal(rng, shape, jnp.float32) * width
    if len(pieces) > 0:
        values = steps_of(rng, shape, pieces, -0.22, 0.18) * values
    return jnp.clip(values, min=-reach, max=reach).astype(kind)


def bell_draw_with(rng, shape, spread, reach, shards, heavy, held_as=jnp.bfloat16):
    values = spread * jax.random.normal(rng, shape, jnp.float32)
    if shards:
        values = values * steps_of(rng, shape, shards, -0.22, 0.18)
    return jnp.clip(strengthened(values, jax.random.fold_in(rng, 3), *heavy), -reach, reach).astype(held_as)


def setup_inputs(seed: int = 0) -> dict:
    splits = jax.random.split(jax.random.key(seed), 11)
    elastic_kernel = bell_draw_with(splits[0], (COL_BLOCKS, ROW_GROUPS * ELEM_DEV, ROW_GROUPS, COL_BLOCKS * ELEM_DEV), ELEMENTS ** -0.5, 0.046875, ((0, 32), (2, 8)), (2, 1, 8, 2.0))
    slip_deficit = gaussian(splits[1], (COL_BLOCKS, ROW_GROUPS, ELEM_DEV, MEMBERS), 1.0, 6.0, ((0, 32), (1, 8)), jnp.float32)
    state_variable = jnp.clip(jnp.exp(math.log(5.0) - 3.218876 * jax.random.uniform(splits[2], (COL_BLOCKS, ROW_GROUPS, ELEM_DEV, MEMBERS), jnp.float32) ** steps_of(splits[2], (COL_BLOCKS, ROW_GROUPS, ELEM_DEV, MEMBERS), ((0, 32), (1, 8)), -0.2, 0.2)), 0.2, 5.0)
    step_size = jnp.clip(jnp.exp(jax.random.uniform(splits[3], (MEMBERS,), jnp.float32, math.log(0.02), math.log(0.1))), 0.02, 0.1)
    load_stress = gaussian(splits[4], (COL_BLOCKS, ROW_GROUPS, ELEM_DEV), 1.0, 6.0, ((0, 32), (1, 8)), jnp.float32)
    normal_stress = jnp.clip(jnp.exp(math.log(2.0) - 1.3862944 * jax.random.uniform(splits[5], (COL_BLOCKS, ROW_GROUPS, ELEM_DEV), jnp.float32) ** steps_of(splits[5], (COL_BLOCKS, ROW_GROUPS, ELEM_DEV), ((0, 32), (1, 8)), -0.2, 0.2)), 0.5, 2.0)
    rate_table = jnp.clip(jnp.exp(jax.random.uniform(splits[6], (REGIONS,), jnp.float32, math.log(0.3), math.log(1.0))), 0.3, 1.0)
    evolve_table = jnp.clip(jnp.exp(jax.random.uniform(splits[7], (REGIONS,), jnp.float32, math.log(0.3), math.log(1.5))), 0.3, 1.5)
    patch_region = touch_ends(jax.random.randint(splits[8], (COL_BLOCKS, ROW_GROUPS, ELEM_DEV), 0, REGIONS), jax.random.fold_in(splits[8], 1), 0, REGIONS - 1).astype(jnp.int32)
    creep_flag = touch_ends((jax.random.randint(splits[9], (COL_BLOCKS, ROW_GROUPS, ELEM_DEV), 0, 4) < 1).astype(jnp.int32), jax.random.fold_in(splits[9], 1), 0, 1)
    return {"elastic_kernel": elastic_kernel, "slip_deficit": slip_deficit, "state_variable": state_variable, "step_size": step_size, "load_stress": load_stress, "normal_stress": normal_stress, "rate_table": rate_table, "evolve_table": evolve_table, "patch_region": patch_region, "creep_flag": creep_flag}


DAMPING = 0.5
PLATE_RATE = 1.0
STEP_CAP = 0.5

def inverse_sinh(value):
    magnitude = jnp.abs(value)
    result = jnp.log(magnitude + jnp.sqrt(magnitude * magnitude + 1.0))
    return jnp.where(value < 0.0, -result, result)

def tractions(elastic_kernel, deficit):
    slip = deficit.astype(jnp.bfloat16)
    sources = jnp.transpose(slip, (1, 0, 2, 3)).reshape(-1, slip.shape[3])

    def one_block(kernel_block):
        flat = kernel_block.reshape(kernel_block.shape[0], -1)
        return jnp.dot(flat, sources, preferred_element_type=jnp.float32)
    result = lax.map(one_block, elastic_kernel)
    return result.reshape(slip.shape)

def solve_rate(stress, pressure, rate_coef, state_coef, state, creeping):
    factor = 0.5 * jnp.exp(state_coef * jnp.log(state) / rate_coef)
    strength = pressure * rate_coef
    speed = stress / (strength * factor + DAMPING)
    for repeat in range(NEWTON):
        scaled = factor * speed
        mismatch = strength * inverse_sinh(scaled) + DAMPING * speed - stress
        gradient = strength * factor / jnp.sqrt(1.0 + scaled * scaled) + DAMPING
        speed = speed - mismatch / gradient
    return jnp.where(creeping, jnp.float32(PLATE_RATE), speed)

def reference(elastic_kernel, slip_deficit, state_variable, step_size, load_stress, normal_stress, rate_table, evolve_table, patch_region, creep_flag):
    levels = jnp.arange(rate_table.shape[0], dtype=jnp.int32)
    onehot = (patch_region[..., None] == levels).astype(jnp.float32)
    rate_coef = lax.optimization_barrier(jnp.sum(onehot * rate_table, axis=-1))[..., None]
    state_coef = lax.optimization_barrier(jnp.sum(onehot * evolve_table, axis=-1))[..., None]
    pressure = normal_stress[..., None]
    loading = load_stress[..., None]
    creeping = (creep_flag == 1)[..., None]
    deficit = slip_deficit
    state = state_variable
    step_now = step_size
    velocity = jnp.zeros_like(deficit)
    for repeat in range(STEPS):
        stress = loading + tractions(elastic_kernel, deficit)
        velocity = solve_rate(stress, pressure, rate_coef, state_coef, state, creeping)
        largest = lax.optimization_barrier(jnp.max(jnp.abs(velocity), axis=(0, 1, 2)))
        state = state * jnp.exp(step_now * (1.0 / state - jnp.abs(velocity)))
        deficit = deficit + step_now * (velocity - PLATE_RATE)
        step_now = STEP_CAP / (1.0 + largest)
    return (velocity, deficit, state, step_now)
```

```python
import functools

import jax
import jax.numpy as jnp
from jax import lax
from jax.experimental import pallas as pl
from jax.experimental.pallas import tpu as pltpu
from jax.sharding import Mesh
from jax.sharding import PartitionSpec as P

NEWTON = 3
BLK = ("yh", "z", "c")
ROW = ("x", "yl")
CHIPS = ("x", "yl", "yh", "z")

DAMPING = 0.5
PLATE_RATE = 1.0
STEP_CAP = 0.5


def inverse_sinh(value):
    magnitude = jnp.abs(value)
    result = jnp.log(magnitude + jnp.sqrt(magnitude * magnitude + 1.0))
    return jnp.where(value < 0.0, -result, result)


def solve_rate(stress, pressure, rate_coef, state_coef, state, creeping):
    factor = 0.5 * jnp.exp(state_coef * jnp.log(state) / rate_coef)
    strength = pressure * rate_coef
    speed = stress / (strength * factor + DAMPING)
    for repeat in range(NEWTON):
        scaled = factor * speed
        mismatch = strength * inverse_sinh(scaled) + DAMPING * speed - stress
        gradient = strength * factor / jnp.sqrt(1.0 + scaled * scaled) + DAMPING
        speed = speed - mismatch / gradient
    return jnp.where(creeping, jnp.float32(PLATE_RATE), speed)


def advance(state, deficit, velocity, step_now):
    new_state = state * jnp.exp(step_now * (1.0 / state - jnp.abs(velocity)))
    new_deficit = deficit + step_now * (velocity - PLATE_RATE)
    return (new_state, new_deficit)


def sort_columns(groups, k_ref, *o_refs):
    width = 2 * k_ref.shape[0]
    piece = 0
    for o_ref in o_refs:
        for part in range(o_ref.shape[1] // width):
            start = pl.multiple_of(groups[piece] * width, width)
            o_ref[:, pl.ds(part * width, width)] = k_ref[:, pl.ds(start, width)]
            piece += 1


def sorted_kernel(kernel_tile, groups, counts, tile):
    rows, columns = kernel_tile.shape
    widths = [count * 2 * tile for count in counts]
    return pl.pallas_call(
        sort_columns,
        grid_spec=pltpu.PrefetchScalarGridSpec(
            num_scalar_prefetch=1,
            grid=(rows // tile,),
            in_specs=[pl.BlockSpec((tile, columns), lambda i, g: (i, 0))],
            out_specs=[pl.BlockSpec((tile, width), lambda i, g: (i, 0)) for width in widths],
        ),
        out_shape=[jax.ShapeDtypeStruct((rows, width), kernel_tile.dtype) for width in widths],
        cost_estimate=pl.CostEstimate(flops=8 << 30, bytes_accessed=16 << 20, transcendentals=0),
    )(groups, kernel_tile)


def swap_cores(x):
    return lax.ppermute(x, "c", ((0, 1), (1, 0)))


def swap_far(x):
    return lax.ppermute(x, "yh", ((0, 1), (1, 0)))


def ring(x, depth):
    pairs = []
    for z in range(depth):
        pairs.append((2 * z, 2 * ((z + 1) % depth)))
        pairs.append((2 * z + 1, 2 * ((z - 1) % depth) + 1))
    return lax.ppermute(x, ("z", "c"), pairs)


def body(
    elastic_kernel,
    slip_deficit,
    state_variable,
    step_size,
    load_stress,
    normal_stress,
    rate_table,
    evolve_table,
    patch_region,
    creep_flag,
):
    kernel_tile = elastic_kernel.reshape(elastic_kernel.shape[1], elastic_kernel.shape[3])
    elements = slip_deficit.shape[2]
    members = slip_deficit.shape[3]
    core = lax.axis_index("c")
    depth = lax.axis_size("z")
    here = lax.axis_index("z")
    near = lax.axis_index("yh")
    first = core == 0

    levels = jnp.arange(rate_table.shape[0], dtype=jnp.int32)
    region = patch_region.reshape(elements)
    onehot = (region[:, None] == levels).astype(jnp.float32)
    rate_coef = jnp.sum(onehot * rate_table, axis=-1)[:, None]
    state_coef = jnp.sum(onehot * evolve_table, axis=-1)[:, None]
    pressure = normal_stress.reshape(elements, 1)
    loading = load_stress.reshape(elements, 1)
    creeping = (creep_flag == 1).reshape(elements, 1)

    back = jnp.where(first, -1, 1)

    def group(side, shift):
        return side * depth + lax.rem(here + shift + depth, depth)

    order = [group(near, 0), group(1 - near, 0)]
    for hop in (1, 2, 3):
        order += [group(near, back * hop), group(1 - near, back * hop)]
    for hop in (1, 2, 3):
        order += [group(near, -back * hop), group(1 - near, -back * hop)]
    flip = jnp.where(first, near, 1 - near)
    order += [group(flip, depth // 2), group(1 - flip, depth // 2)]
    counts = (2, 4, 8, 2)
    tiles = sorted_kernel(kernel_tile, jnp.stack(order).astype(jnp.int32), counts, elements)

    def paired(mine, other):
        return jnp.where(first, jnp.concatenate([mine, other]), jnp.concatenate([other, mine]))

    def gathered(block):
        far = swap_far(block)
        a = paired(block, swap_cores(block))
        b = paired(far, swap_cores(far))
        pieces = [a, b]
        for hop in (1, 2, 3):
            a, b = ring(a, depth), ring(b, depth)
            pieces += [a, b]
        half = jnp.where(first, a, b)
        held = lax.optimization_barrier((half, *pieces[2:]))
        last = ring(held[0], depth)
        pieces += [swap_cores(piece) for piece in held[1:]]
        pieces += [last, swap_cores(last)]
        return pieces

    def slips_of(pieces, span):
        return jnp.concatenate(
            [piece[at : at + elements] for piece in pieces for at in (0, span)]
        )

    def partial_of(pieces, span):
        partial = None
        at = 0
        for count, tile in zip(counts, tiles):
            slips = slips_of(pieces[at : at + count], span)
            at += count
            term = jnp.dot(tile, slips, preferred_element_type=jnp.float32)
            partial = term if partial is None else lax.optimization_barrier(partial + term)
        return partial.astype(jnp.bfloat16).reshape(-1, elements, members)

    def summed(parts):
        return jnp.sum(parts.astype(jnp.float32), axis=0)

    def exchanged(parts):
        return lax.all_to_all(parts, ROW, 0, 0, tiled=True)

    def solved(traction, state):
        return solve_rate(loading + traction, pressure, rate_coef, state_coef, state, creeping)

    spare = 8

    def split_rows(largest):
        high = largest.astype(jnp.bfloat16)
        rest = largest - high.astype(jnp.float32)
        low = rest.astype(jnp.bfloat16)
        return jnp.concatenate(
            [high[None], low[None], jnp.zeros((spare - 2, members), jnp.bfloat16)]
        )

    def joined_rows(rows):
        return jnp.max(rows[:, 0].astype(jnp.float32) + rows[:, 1].astype(jnp.float32), axis=0)

    def largest_of(local):
        half = members // 2
        mine = jnp.where(first, local[:half], local[half:])
        other = jnp.where(first, local[half:], local[:half])
        mine = jnp.maximum(mine, swap_cores(other))
        chips = functools.reduce(lambda n, axis: n * lax.axis_size(axis), CHIPS, 1)
        everyone = lax.all_to_all(
            jnp.broadcast_to(mine, (chips, half)), CHIPS, 0, 0, tiled=True
        )
        mine = jnp.max(everyone, axis=0)
        other = swap_cores(mine)
        return jnp.where(first, jnp.concatenate([mine, other]), jnp.concatenate([other, mine]))

    deficit = slip_deficit.reshape(elements, members)
    state = state_variable.reshape(elements, members)

    pieces = gathered(deficit.astype(jnp.bfloat16))
    traction = summed(exchanged(partial_of(pieces, elements)))
    velocity = solved(traction, state)
    local = jnp.max(jnp.abs(velocity), axis=0)
    state, deficit = advance(state, deficit, velocity, step_size)

    rows = split_rows(local)
    pieces = gathered(jnp.concatenate([deficit.astype(jnp.bfloat16), rows]))
    span = elements + spare
    parts = partial_of(pieces, span)
    rows = [piece[at : at + spare] for piece in pieces for at in (elements, span + elements)]
    rows = split_rows(joined_rows(jnp.stack(rows)))
    rows = jnp.broadcast_to(rows, (parts.shape[0], *rows.shape))
    parts = exchanged(jnp.concatenate([parts, rows], axis=1))
    velocity = solved(summed(parts[:, :elements]), state)
    local = jnp.max(jnp.abs(velocity), axis=0)
    largest = joined_rows(parts[:, elements:])
    state, deficit = advance(state, deficit, velocity, STEP_CAP / (1.0 + largest))
    step_next = STEP_CAP / (1.0 + largest_of(local))
    shape = slip_deficit.shape
    return (velocity.reshape(shape), deficit.reshape(shape), state.reshape(shape), step_next)


def solution(mesh):
    torus = Mesh(mesh.devices.reshape(4, 2, 2, 8, 2), ("x", "yl", "yh", "z", "c"))
    in_specs = (
        P(BLK, None, ROW, None),
        P(BLK, ROW, None, None),
        P(BLK, ROW, None, None),
        P(),
        P(BLK, ROW, None),
        P(BLK, ROW, None),
        P(),
        P(),
        P(BLK, ROW, None),
        P(BLK, ROW, None),
    )
    out_specs = (P(BLK, ROW, None, None), P(BLK, ROW, None, None), P(BLK, ROW, None, None), P())
    return jax.shard_map(body, mesh=torus, in_specs=in_specs, out_specs=out_specs, check_vma=False)
```

```python
import functools

import jax
import jax.numpy as jnp
from jax import lax
from jax.sharding import Mesh
from jax.sharding import PartitionSpec as P


NEWTON = 3
STEPS = 2
BLK = ("yh", "z", "c")
ROW = ("x", "yl")
CHIPS = ("x", "yl", "yh", "z")

DAMPING = 0.5
PLATE_RATE = 1.0
STEP_CAP = 0.5


def inverse_sinh(value):
    magnitude = jnp.abs(value)
    result = jnp.log(magnitude + jnp.sqrt(magnitude * magnitude + 1.0))
    return jnp.where(value < 0.0, -result, result)


def solve_rate(stress, pressure, rate_coef, state_coef, state, creeping):
    factor = 0.5 * jnp.exp(state_coef * jnp.log(state) / rate_coef)
    strength = pressure * rate_coef
    speed = stress / (strength * factor + DAMPING)
    for _ in range(NEWTON):
        scaled = factor * speed
        mismatch = strength * inverse_sinh(scaled) + DAMPING * speed - stress
        gradient = strength * factor / jnp.sqrt(1.0 + scaled * scaled) + DAMPING
        speed = speed - mismatch / gradient
    return jnp.where(creeping, jnp.float32(PLATE_RATE), speed)


def advance(state, deficit, velocity, step_now):
    new_state = state * jnp.exp(step_now * (1.0 / state - jnp.abs(velocity)))
    new_deficit = deficit + step_now * (velocity - PLATE_RATE)
    return (new_state, new_deficit)


def swap_cores(x):
    return lax.ppermute(x, "c", ((0, 1), (1, 0)))


def swap_far(x):
    return lax.ppermute(x, "yh", ((0, 1), (1, 0)))


def shifted(x, by):
    depth = lax.axis_size("z")
    return lax.ppermute(x, "z", [(z, (z + by) % depth) for z in range(depth)])


def body(
    elastic_kernel,
    slip_deficit,
    state_variable,
    step_size,
    load_stress,
    normal_stress,
    rate_table,
    evolve_table,
    patch_region,
    creep_flag,
):
    kernel_tile = elastic_kernel.reshape(elastic_kernel.shape[1], elastic_kernel.shape[3])
    elements = slip_deficit.shape[2]
    members = slip_deficit.shape[3]
    core = lax.axis_index("c")
    depth = lax.axis_size("z")
    here = lax.axis_index("z")
    near = lax.axis_index("yh")
    first = core == 0

    fault = (rate_table, evolve_table, patch_region, creep_flag, normal_stress, load_stress)

    def coefs_of(fault):
        rate_table, evolve_table, patch_region, creep_flag, normal_stress, load_stress = fault
        levels = jnp.arange(rate_table.shape[0], dtype=jnp.int32)
        onehot = (patch_region.reshape(elements)[:, None] == levels).astype(jnp.float32)
        rate_coef = jnp.sum(onehot * rate_table, axis=-1)[:, None]
        state_coef = jnp.sum(onehot * evolve_table, axis=-1)[:, None]
        pressure = normal_stress.reshape(elements, 1)
        loading = load_stress.reshape(elements, 1)
        creeping = creep_flag.reshape(elements, 1)
        return (rate_coef, state_coef, pressure, loading, creeping)

    half = depth * 2 * elements

    def tile_of(side):
        return lax.dynamic_slice(kernel_tile, (0, side * half), (kernel_tile.shape[0], half))

    def swapped(blocks):
        both = swap_cores(jnp.concatenate([block for _, block in blocks]))
        span = blocks[0][1].shape[0]
        return [(shift, both[i * span : (i + 1) * span]) for i, (shift, _) in enumerate(blocks)]

    def after(blocks, token):
        held, _ = lax.optimization_barrier(([block for _, block in blocks], token))
        return [(shift, block) for (shift, _), block in zip(blocks, held)]

    def joined(rows):
        return rows[0].astype(jnp.float32) + rows[1].astype(jnp.float32)

    def gathered(block):
        found = [joined(block[elements:])]

        def marked(block, by):
            block = shifted(block, by)
            found.append(joined(block[elements:]))
            return block

        far = swap_far(block)
        found.append(joined(far[elements:]))
        start = [[(0, block)], [(0, far)]]
        up, down = [block, far], [block, far]
        hops = [[], []]
        for hop in (1, 2, 3):
            for side in (0, 1):
                up[side] = marked(up[side], 1)
                down[side] = marked(down[side], -1)
                hops[side].append([(-hop, up[side]), (hop, down[side])])
        last = [[(4, marked(up[0], 1))], [(4, marked(down[1], -1))]]
        mine = [start[side] + sum(hops[side], []) + last[side] for side in (0, 1)]
        token = (up[0], down[0], up[1], down[1])
        other = [
            swapped(after(start[side] + hops[side][0] + hops[side][1], token))
            for side in (0, 1)
        ]
        other[0] += swapped(hops[0][2] + last[0])
        other[1] += swapped(hops[1][2]) + swapped(last[1])
        found += [joined(block[elements:]) for side in other for _, block in side]
        return mine, other, found

    def placed(mine, other):
        slips = jnp.zeros((half, members), jnp.bfloat16)
        for owner_core, blocks in ((core, mine), (1 - core, other)):
            for shift, block in blocks:
                owner = 2 * lax.rem(here + shift + depth, depth) + owner_core
                slips = lax.dynamic_update_slice(slips, block[:elements], (owner * elements, 0))
        return slips

    def partial_of(mine, other, side):
        slips = placed(mine[0], other[0])
        partial = jnp.dot(tile_of(side), slips, preferred_element_type=jnp.float32)
        (shift, block) = other[1][-1]
        partial, block = lax.optimization_barrier((partial, block))
        slips = placed(mine[1], [*other[1][:-1], (shift, block)])
        partial += jnp.dot(tile_of(1 - side), slips, preferred_element_type=jnp.float32)
        return partial.astype(jnp.bfloat16).reshape(-1, elements, members)

    def summed(parts):
        return jnp.sum(parts.astype(jnp.float32), axis=0)

    def exchanged(parts):
        return lax.all_to_all(parts, ROW, 0, 0, tiled=True)

    def solved(traction, state, coefs):
        rate_coef, state_coef, pressure, loading, creeping = coefs
        stress = loading + traction
        return solve_rate(stress, pressure, rate_coef, state_coef, state, creeping == 1)

    spare = 8

    def split_rows(largest):
        high = largest.astype(jnp.bfloat16)
        rest = largest - high.astype(jnp.float32)
        low = rest.astype(jnp.bfloat16)
        return jnp.concatenate(
            [high[None], low[None], jnp.zeros((spare - 2, members), jnp.bfloat16)]
        )

    def largest_of(local):
        count = members // 2
        mine = jnp.where(first, local[:count], local[count:])
        other = jnp.where(first, local[count:], local[:count])
        mine = jnp.maximum(mine, swap_cores(other))
        chips = functools.reduce(lambda n, axis: n * lax.axis_size(axis), CHIPS, 1)
        everyone = lax.all_to_all(
            jnp.broadcast_to(mine, (chips, count)), CHIPS, 0, 0, tiled=True
        )
        mine = jnp.max(everyone, axis=0)
        other = swap_cores(mine)
        return jnp.where(first, jnp.concatenate([mine, other]), jnp.concatenate([other, mine]))

    def step(carry):
        index, deficit, state, _, local = carry
        deficit = jnp.where(index == 0, slip_deficit.reshape(elements, members), deficit)
        state = jnp.where(index == 0, state_variable.reshape(elements, members), state)
        block = jnp.concatenate([deficit.astype(jnp.bfloat16), split_rows(local)])
        mine, other, found = gathered(block)
        side, held, _ = lax.optimization_barrier((near, fault, index))
        coefs = coefs_of(held)
        parts = partial_of(mine, other, side)
        rows = split_rows(functools.reduce(jnp.maximum, found))
        rows = jnp.broadcast_to(rows, (parts.shape[0], *rows.shape))
        parts = jnp.concatenate([parts, rows], axis=1)
        held = (coefs, deficit, state, index)
        parts, held = lax.optimization_barrier((parts, held))
        parts, held = lax.optimization_barrier((exchanged(parts), held))
        coefs, deficit, state, index = held
        velocity = solved(summed(parts[:, :elements]), state, coefs)
        local = jnp.max(jnp.abs(velocity), axis=0)
        found = [joined(parts[row, elements:]) for row in range(parts.shape[0])]
        largest = functools.reduce(jnp.maximum, found)
        step_now = jnp.where(index == 0, step_size, STEP_CAP / (1.0 + largest))
        state, deficit = advance(state, deficit, velocity, step_now)
        return index + 1, deficit, state, velocity, local

    blank = jnp.zeros((elements, members), jnp.float32)
    carry = (jnp.int32(0), blank, blank, blank, jnp.zeros((members,), jnp.float32))
    carry = lax.while_loop(lambda carry: carry[0] < STEPS, step, carry)
    _, deficit, state, velocity, local = carry
    step_next = STEP_CAP / (1.0 + largest_of(local))
    shape = slip_deficit.shape
    return (velocity.reshape(shape), deficit.reshape(shape), state.reshape(shape), step_next)


def solution(mesh):
    torus = Mesh(mesh.devices.reshape(4, 2, 2, 8, 2), ("x", "yl", "yh", "z", "c"))
    in_specs = (
        P(BLK, None, ROW, None),
        P(BLK, ROW, None, None),
        P(BLK, ROW, None, None),
        P(),
        P(BLK, ROW, None),
        P(BLK, ROW, None),
        P(),
        P(),
        P(BLK, ROW, None),
        P(BLK, ROW, None),
    )
    out_specs = (P(BLK, ROW, None, None), P(BLK, ROW, None, None), P(BLK, ROW, None, None), P())
    return jax.shard_map(body, mesh=torus, in_specs=in_specs, out_specs=out_specs, check_vma=False)
```

```python
import functools

import jax
import jax.numpy as jnp
from jax import lax
from jax.sharding import Mesh
from jax.sharding import PartitionSpec as P


NEWTON = 3
STEPS = 2
BLK = ("yh", "z", "c")
ROW = ("x", "yl")
CHIPS = ("x", "yl", "yh", "z")

DAMPING = 0.5
PLATE_RATE = 1.0
STEP_CAP = 0.5


def inverse_sinh(value):
    magnitude = jnp.abs(value)
    result = jnp.log(magnitude + jnp.sqrt(magnitude * magnitude + 1.0))
    return jnp.where(value < 0.0, -result, result)


def solve_rate(stress, pressure, rate_coef, state_coef, state, creeping):
    factor = 0.5 * jnp.exp(state_coef * jnp.log(state) / rate_coef)
    strength = pressure * rate_coef
    speed = stress / (strength * factor + DAMPING)
    for _ in range(NEWTON):
        scaled = factor * speed
        mismatch = strength * inverse_sinh(scaled) + DAMPING * speed - stress
        gradient = strength * factor / jnp.sqrt(1.0 + scaled * scaled) + DAMPING
        speed = speed - mismatch / gradient
    return jnp.where(creeping, jnp.float32(PLATE_RATE), speed)


def advance(state, deficit, velocity, step_now):
    new_state = state * jnp.exp(step_now * (1.0 / state - jnp.abs(velocity)))
    new_deficit = deficit + step_now * (velocity - PLATE_RATE)
    return (new_state, new_deficit)


def swap_cores(x):
    return lax.ppermute(x, "c", ((0, 1), (1, 0)))


def swap_far(x):
    return lax.ppermute(x, "yh", ((0, 1), (1, 0)))


def shifted(x, by):
    depth = lax.axis_size("z")
    return lax.ppermute(x, "z", [(z, (z + by) % depth) for z in range(depth)])


def body(
    elastic_kernel,
    slip_deficit,
    state_variable,
    step_size,
    load_stress,
    normal_stress,
    rate_table,
    evolve_table,
    patch_region,
    creep_flag,
):
    kernel_tile = elastic_kernel.reshape(elastic_kernel.shape[1], elastic_kernel.shape[3])
    elements = slip_deficit.shape[2]
    members = slip_deficit.shape[3]
    core = lax.axis_index("c")
    depth = lax.axis_size("z")
    here = lax.axis_index("z")
    near = lax.axis_index("yh")

    fault = (rate_table, evolve_table, patch_region, creep_flag, normal_stress, load_stress)

    def coefs_of(fault):
        rate_table, evolve_table, patch_region, creep_flag, normal_stress, load_stress = fault
        levels = jnp.arange(rate_table.shape[0], dtype=jnp.int32)
        onehot = (patch_region.reshape(elements)[:, None] == levels).astype(jnp.float32)
        rate_coef = jnp.sum(onehot * rate_table, axis=-1)[:, None]
        state_coef = jnp.sum(onehot * evolve_table, axis=-1)[:, None]
        pressure = normal_stress.reshape(elements, 1)
        loading = load_stress.reshape(elements, 1)
        creeping = creep_flag.reshape(elements, 1)
        return (rate_coef, state_coef, pressure, loading, creeping)

    half = depth * 2 * elements

    def tile_of(side):
        return lax.dynamic_slice(kernel_tile, (0, side * half), (kernel_tile.shape[0], half))

    def swapped(blocks):
        both = swap_cores(jnp.concatenate([block for _, block in blocks]))
        span = blocks[0][1].shape[0]
        return [(shift, both[i * span : (i + 1) * span]) for i, (shift, _) in enumerate(blocks)]

    def after(blocks, token):
        held, _ = lax.optimization_barrier(([block for _, block in blocks], token))
        return [(shift, block) for (shift, _), block in zip(blocks, held)]

    def joined(rows):
        return rows[0].astype(jnp.float32) + rows[1].astype(jnp.float32)

    def gathered(block):
        found = [joined(block[elements:])]

        def marked(block, by):
            block = shifted(block, by)
            found.append(joined(block[elements:]))
            return block

        far = swap_far(block)
        found.append(joined(far[elements:]))
        start = [[(0, block)], [(0, far)]]
        up, down = [block, far], [block, far]
        hops = [[], []]
        for hop in (1, 2, 3):
            for side in (0, 1):
                up[side] = marked(up[side], 1)
                down[side] = marked(down[side], -1)
                hops[side].append([(-hop, up[side]), (hop, down[side])])
        last = [[(4, marked(up[0], 1))], [(4, marked(down[1], -1))]]
        mine = [start[side] + sum(hops[side], []) + last[side] for side in (0, 1)]
        token = (up[0], down[0], up[1], down[1])
        other = [
            swapped(after(start[side] + hops[side][0] + hops[side][1], token))
            for side in (0, 1)
        ]
        other[0] += swapped(hops[0][2] + last[0])
        other[1] += swapped(hops[1][2]) + swapped(last[1])
        found += [joined(block[elements:]) for side in other for _, block in side]
        return mine, other, found

    def placed(mine, other, blank):
        slips = blank
        for owner_core, blocks in ((core, mine), (1 - core, other)):
            for shift, block in blocks:
                owner = 2 * lax.rem(here + shift + depth, depth) + owner_core
                block = block[:elements].reshape(-1, *blank.shape[1:])
                start = (owner * block.shape[0], *(0 for _ in blank.shape[1:]))
                slips = lax.dynamic_update_slice(slips, block, start)
        return slips.reshape(half, members)

    def partial_of(mine, other, side):
        near_blank = jnp.zeros((half, members), jnp.bfloat16)
        far_blank = jnp.zeros((half // elements, elements, members), jnp.bfloat16)
        slips = placed(mine[0], other[0], near_blank)
        partial = jnp.dot(tile_of(side), slips, preferred_element_type=jnp.float32)
        partial = lax.optimization_barrier(partial)
        slips = placed(mine[1], other[1], far_blank)
        partial += jnp.dot(tile_of(1 - side), slips, preferred_element_type=jnp.float32)
        return partial.astype(jnp.bfloat16).reshape(-1, elements, members)

    def summed(parts):
        return jnp.sum(parts.astype(jnp.float32), axis=0)

    def exchanged(parts):
        return lax.all_to_all(parts, ROW, 0, 0, tiled=True)

    def solved(traction, state, coefs):
        rate_coef, state_coef, pressure, loading, creeping = coefs
        stress = loading + traction
        return solve_rate(stress, pressure, rate_coef, state_coef, state, creeping == 1)

    spare = 8

    def split_rows(largest):
        high = largest.astype(jnp.bfloat16)
        rest = largest - high.astype(jnp.float32)
        low = rest.astype(jnp.bfloat16)
        return jnp.concatenate(
            [high[None], low[None], jnp.zeros((spare - 2, members), jnp.bfloat16)]
        )

    def largest_of(local):
        local = jnp.maximum(local, swap_cores(local))
        chips = functools.reduce(lambda n, axis: n * lax.axis_size(axis), CHIPS, 1)
        everyone = jnp.broadcast_to(local, (chips, members))
        return jnp.max(lax.all_to_all(everyone, CHIPS, 0, 0, tiled=True), axis=0)

    def step(carry):
        index, deficit, state, _, local = carry
        block = jnp.concatenate([deficit.astype(jnp.bfloat16), split_rows(local)])
        mine, other, found = gathered(block)
        side, held, _ = lax.optimization_barrier((near, fault, index))
        coefs = coefs_of(held)
        parts = partial_of(mine, other, side)
        rows = split_rows(functools.reduce(jnp.maximum, found))
        rows = jnp.broadcast_to(rows, (parts.shape[0], *rows.shape))
        parts = jnp.concatenate([parts, rows], axis=1)
        held = (coefs, deficit, state, state_variable, index)
        parts, held = lax.optimization_barrier((parts, held))
        parts, held = lax.optimization_barrier((exchanged(parts), held))
        coefs, deficit, state, begin, index = held
        state = jnp.where(index == 0, begin.reshape(elements, members), state)
        velocity = solved(summed(parts[:, :elements]), state, coefs)
        local = jnp.max(jnp.abs(velocity), axis=0)
        found = [joined(parts[row, elements:]) for row in range(parts.shape[0])]
        largest = functools.reduce(jnp.maximum, found)
        step_now = jnp.where(index == 0, step_size, STEP_CAP / (1.0 + largest))
        state, deficit = advance(state, deficit, velocity, step_now)
        return index + 1, deficit, state, velocity, local

    blank = jnp.zeros((elements, members), jnp.float32)
    deficit = slip_deficit.reshape(elements, members)
    carry = (jnp.int32(0), deficit, blank, blank, jnp.zeros((members,), jnp.float32))
    carry = lax.while_loop(lambda carry: carry[0] < STEPS, step, carry)
    _, deficit, state, velocity, local = carry
    step_next = STEP_CAP / (1.0 + largest_of(local))
    shape = slip_deficit.shape
    return (velocity.reshape(shape), deficit.reshape(shape), state.reshape(shape), step_next)


def solution(mesh):
    torus = Mesh(mesh.devices.reshape(4, 2, 2, 8, 2), ("x", "yl", "yh", "z", "c"))
    in_specs = (
        P(BLK, None, ROW, None),
        P(BLK, ROW, None, None),
        P(BLK, ROW, None, None),
        P(),
        P(BLK, ROW, None),
        P(BLK, ROW, None),
        P(),
        P(),
        P(BLK, ROW, None),
        P(BLK, ROW, None),
    )
    out_specs = (P(BLK, ROW, None, None), P(BLK, ROW, None, None), P(BLK, ROW, None, None), P())
    return jax.shard_map(body, mesh=torus, in_specs=in_specs, out_specs=out_specs, check_vma=False)
```

```python
import functools

import jax
import jax.numpy as jnp
from jax import lax
from jax.sharding import Mesh
from jax.sharding import PartitionSpec as P


NEWTON = 3
STEPS = 2
BLK = ("yh", "z", "c")
ROW = ("x", "yl")
CHIPS = ("x", "yl", "yh", "z")

DAMPING = 0.5
PLATE_RATE = 1.0
STEP_CAP = 0.5


def inverse_sinh(value):
    magnitude = jnp.abs(value)
    result = jnp.log(magnitude + jnp.sqrt(magnitude * magnitude + 1.0))
    return jnp.where(value < 0.0, -result, result)


def solve_rate(stress, pressure, rate_coef, state_coef, state, creeping):
    factor = 0.5 * jnp.exp(state_coef * jnp.log(state) / rate_coef)
    strength = pressure * rate_coef
    speed = stress / (strength * factor + DAMPING)
    for _ in range(NEWTON):
        scaled = factor * speed
        mismatch = strength * inverse_sinh(scaled) + DAMPING * speed - stress
        gradient = strength * factor / jnp.sqrt(1.0 + scaled * scaled) + DAMPING
        speed = speed - mismatch / gradient
    return jnp.where(creeping, jnp.float32(PLATE_RATE), speed)


def advance(state, deficit, velocity, step_now):
    new_state = state * jnp.exp(step_now * (1.0 / state - jnp.abs(velocity)))
    new_deficit = deficit + step_now * (velocity - PLATE_RATE)
    return (new_state, new_deficit)


def swap_cores(x):
    return lax.ppermute(x, "c", ((0, 1), (1, 0)))


def swap_far(x):
    return lax.ppermute(x, "yh", ((0, 1), (1, 0)))


def shifted(x, by):
    depth = lax.axis_size("z")
    return lax.ppermute(x, "z", [(z, (z + by) % depth) for z in range(depth)])


def body(
    elastic_kernel,
    slip_deficit,
    state_variable,
    step_size,
    load_stress,
    normal_stress,
    rate_table,
    evolve_table,
    patch_region,
    creep_flag,
):
    kernel_tile = elastic_kernel.reshape(elastic_kernel.shape[1], elastic_kernel.shape[3])
    elements = slip_deficit.shape[2]
    members = slip_deficit.shape[3]
    core = lax.axis_index("c")
    depth = lax.axis_size("z")
    here = lax.axis_index("z")
    near = lax.axis_index("yh")

    fault = (rate_table, evolve_table, patch_region, creep_flag, normal_stress, load_stress)

    def coefs_of(fault):
        rate_table, evolve_table, patch_region, creep_flag, normal_stress, load_stress = fault
        levels = jnp.arange(rate_table.shape[0], dtype=jnp.int32)
        onehot = (patch_region.reshape(elements)[:, None] == levels).astype(jnp.float32)
        rate_coef = jnp.sum(onehot * rate_table, axis=-1)[:, None]
        state_coef = jnp.sum(onehot * evolve_table, axis=-1)[:, None]
        pressure = normal_stress.reshape(elements, 1)
        loading = load_stress.reshape(elements, 1)
        creeping = creep_flag.reshape(elements, 1)
        return (rate_coef, state_coef, pressure, loading, creeping)

    half = depth * 2 * elements

    def tile_of(side):
        return lax.dynamic_slice(kernel_tile, (0, side * half), (kernel_tile.shape[0], half))

    def swapped(blocks):
        both = swap_cores(jnp.concatenate([block for _, block in blocks]))
        span = blocks[0][1].shape[0]
        return [(shift, both[i * span : (i + 1) * span]) for i, (shift, _) in enumerate(blocks)]

    def after(blocks, token):
        held, _ = lax.optimization_barrier(([block for _, block in blocks], token))
        return [(shift, block) for (shift, _), block in zip(blocks, held)]

    def gathered(block):
        slips = [
            jnp.zeros((half, members), jnp.bfloat16),
            jnp.zeros((half // elements, elements, members), jnp.bfloat16),
        ]

        def place(side, owner_core, shift, block):
            owner = 2 * lax.rem(here + shift + depth, depth) + owner_core
            if side == 0:
                slips[0] = lax.dynamic_update_slice(slips[0], block, (owner * elements, 0))
            else:
                slips[1] = lax.dynamic_update_slice(slips[1], block[None], (owner, 0, 0))

        def hopped(side, shift, block, by):
            block = shifted(block, by)
            place(side, core, shift, block)
            return block

        far = swap_far(block)
        start = [[(0, block)], [(0, far)]]
        place(0, core, 0, block)
        place(1, core, 0, far)
        up, down = [block, far], [block, far]
        hops = [[], []]
        for hop in (1, 2, 3):
            up[0] = hopped(0, -hop, up[0], 1)
            down[0] = hopped(0, hop, down[0], -1)
            down[1] = hopped(1, hop, down[1], -1)
            up[1] = hopped(1, -hop, up[1], 1)
            for side in (0, 1):
                hops[side].append([(-hop, up[side]), (hop, down[side])])
        last = [[(4, hopped(0, 4, up[0], 1))], [(4, hopped(1, 4, down[1], -1))]]
        token = (up[0], down[0], up[1], down[1])
        other = [
            swapped(after(start[side] + hops[side][0] + hops[side][1], token))
            for side in (0, 1)
        ]
        other[0] += swapped(hops[0][2] + last[0])
        other[1] += swapped(hops[1][2]) + swapped(last[1])
        for side in (0, 1):
            for shift, block in other[side]:
                place(side, 1 - core, shift, block)
        return slips[0], slips[1].reshape(half, members)

    def partial_of(slips, side):
        partial = jnp.dot(tile_of(side), slips[0], preferred_element_type=jnp.float32)
        partial = lax.optimization_barrier(partial)
        partial += jnp.dot(tile_of(1 - side), slips[1], preferred_element_type=jnp.float32)
        return partial.astype(jnp.bfloat16).reshape(-1, elements, members)

    def summed(parts):
        return jnp.sum(parts.astype(jnp.float32), axis=0)

    def exchanged(parts):
        return lax.all_to_all(parts, ROW, 0, 0, tiled=True)

    def solved(traction, state, coefs):
        rate_coef, state_coef, pressure, loading, creeping = coefs
        stress = loading + traction
        return solve_rate(stress, pressure, rate_coef, state_coef, state, creeping == 1)

    def largest_of(local):
        local = local.astype(jnp.bfloat16)
        local = jnp.maximum(local, swap_cores(local))
        chips = functools.reduce(lambda n, axis: n * lax.axis_size(axis), CHIPS, 1)
        everyone = jnp.broadcast_to(local, (chips, *local.shape))
        everyone = lax.all_to_all(everyone, CHIPS, 0, 0, tiled=True)
        return jnp.max(everyone, axis=0).astype(jnp.float32)

    def step(carry):
        index, deficit, state, velocity, _, local = carry
        step_now = jnp.where(index == 0, 0.0, step_size)
        _, deficit = advance(state, deficit, velocity, step_now)
        slips = gathered(deficit.astype(jnp.bfloat16))
        side, held, _ = lax.optimization_barrier((near, fault, index))
        coefs = coefs_of(held)
        parts = partial_of(slips, side)
        held = (coefs, deficit, state, state_variable, velocity, local, index)
        parts, held = lax.optimization_barrier((parts, held))
        parts, held = lax.optimization_barrier((exchanged(parts), held))
        coefs, deficit, state, begin, velocity, local, index = held
        state, _ = advance(state, deficit, velocity, step_size)
        state = jnp.where(index == 0, begin.reshape(elements, members), state)
        velocity = solved(summed(parts), state, coefs)
        return index + 1, deficit, state, velocity, local, jnp.max(jnp.abs(velocity), axis=0)

    blank = jnp.zeros((members,), jnp.float32)
    deficit = slip_deficit.reshape(elements, members)
    carry = (jnp.int32(0), deficit, jnp.ones_like(deficit), jnp.zeros_like(deficit), blank, blank)
    carry = lax.while_loop(lambda carry: carry[0] < STEPS, step, carry)
    _, deficit, state, velocity, local_first, local_second = carry
    largest = largest_of(jnp.stack([local_first, local_second]))
    state, deficit = advance(state, deficit, velocity, STEP_CAP / (1.0 + largest[0]))
    step_next = STEP_CAP / (1.0 + largest[1])
    shape = slip_deficit.shape
    return (velocity.reshape(shape), deficit.reshape(shape), state.reshape(shape), step_next)


def solution(mesh):
    torus = Mesh(mesh.devices.reshape(4, 2, 2, 8, 2), ("x", "yl", "yh", "z", "c"))
    in_specs = (
        P(BLK, None, ROW, None),
        P(BLK, ROW, None, None),
        P(BLK, ROW, None, None),
        P(),
        P(BLK, ROW, None),
        P(BLK, ROW, None),
        P(),
        P(),
        P(BLK, ROW, None),
        P(BLK, ROW, None),
    )
    out_specs = (P(BLK, ROW, None, None), P(BLK, ROW, None, None), P(BLK, ROW, None, None), P())
    return jax.shard_map(body, mesh=torus, in_specs=in_specs, out_specs=out_specs, check_vma=False)
```
